32 devices in a mesh: dp: 2 (over x), sp: 16 (over y, z, core).
Axes of the slice: x: 2, y: 2, z: 4, core: 2. Of those that a mesh axis runs over, the one named last changes fastest.
Arguments:
- q: bfloat16 [64, 32, 80], P('dp'), parts along dimension 0
- k: bfloat16 [64, 4096, 32, 80], P('dp', 'sp'), parts along dimension 0
- v: bfloat16 [64, 4096, 32, 80], P('dp', 'sp'), parts along dimension 0
Outputs:
- q: bfloat16 [64, 32, 80], P('dp'), parts along dimension 0
There are 2 independent parts. The reference program is written for one: setup_inputs(seed, part) draws one part's arguments, and reference() takes and returns one part's arrays. A program takes and returns all parts, laid end to end along the dimension named above; each array names one.
All inputs are finite; a program needn't handle non-finite values.
Results may differ from the reference program's by a relative error of at most 0.012.
Values are sent between devices in bfloat16 or wider.
A program may use at most 2 GiB of HBM per device.

```python
import jax
import jax.numpy as jnp

BATCH = 32
CACHE = 4096
HEADS = 32
KV_HEADS = 32
HEAD = 80


def setup_inputs(seed: int = 0, part: int = 0) -> dict:
    kq, kk, kv = (jax.random.fold_in(k, part) for k in jax.random.split(jax.random.key(seed), 3))
    return {
        "q": (3 * jax.random.normal(kq, (BATCH, HEADS, HEAD), jnp.float32)).astype(jnp.bfloat16),
        "k": jax.random.normal(kk, (BATCH, CACHE, KV_HEADS, HEAD), jnp.float32).astype(jnp.bfloat16),
        "v": jax.random.normal(kv, (BATCH, CACHE, KV_HEADS, HEAD), jnp.float32).astype(jnp.bfloat16),
    }


def einsum(form, a, b):
    return jnp.einsum(form, a.astype(jnp.float32), b.astype(jnp.float32))


def reference(q, k, v):
    grouped = q.reshape(BATCH, KV_HEADS, -1, HEAD)
    scores = einsum("bgsd,bugd->bgsu", grouped, k) * HEAD**-0.5
    weights = jax.nn.softmax(scores, -1).astype(jnp.bfloat16)
    return einsum("bgsu,bugd->bgsd", weights, v).astype(jnp.bfloat16).reshape(BATCH, HEADS, HEAD)
```

```python
import functools

import jax
import jax.numpy as jnp
from jax import lax
from jax.experimental import pallas as pl
from jax.experimental.pallas import tpu as pltpu
from jax.sharding import PartitionSpec as P

SLOTS = 8
LANES = 128


def owner_chip(b):
    return lax.rem(3 * lax.rem(b, 8) + 4, 8)


def kernel(scale, q_ref, k_hbm, v_hbm, out_ref, kbuf, vbuf, mask, qpad, turned, weights, stats, send, recv,
           ksem, vsem, rs_send, rs_recv, ag_send, ag_recv):
    batches, heads, head = q_ref.shape
    tokens = k_hbm.shape[-1]
    half = heads // 2
    n = 16
    me = lax.axis_index("sp")
    my_chip, my_core = me // 2, lax.rem(me, 2)

    def fetch(hbm, buf, sem, b):
        return pltpu.make_async_copy(hbm.at[b], buf.at[lax.rem(b, SLOTS)], sem.at[lax.rem(b, SLOTS)])

    for b in range(SLOTS):
        fetch(k_hbm, kbuf, ksem, b).start()
        fetch(v_hbm, vbuf, vsem, b).start()

    barrier = pltpu.get_barrier_semaphore()
    for d in range(1, n):
        pl.semaphore_signal(barrier, 1, device_id={"sp": lax.rem(me + d, n)}, device_id_type=pl.DeviceIdType.MESH)

    row = lax.broadcasted_iota(jnp.int32, (heads, heads * head), 0)
    col = lax.broadcasted_iota(jnp.int32, (heads, heads * head), 1)
    mask[...] = jnp.where((col >= row * head) & (col < row * head + head), 1.0, 0.0).astype(jnp.bfloat16)
    qpad[...] = jnp.zeros_like(qpad)
    lane = lax.broadcasted_iota(jnp.int32, (heads, LANES), 1)
    shift = lax.rem(lax.broadcasted_iota(jnp.int32, (heads, LANES), 0) * head, LANES)

    def turn(i, carry):
        for j in range(2):
            qpad[j, :, :head] = q_ref[2 * i + j].astype(jnp.float32)
            x = qpad[j]
            for bit in (16, 32, 64):
                x = jnp.where((shift & bit) != 0, pltpu.roll(x, bit, 1), x)
            turned[2 * i + j] = x.astype(jnp.bfloat16)
        return carry

    lax.fori_loop(0, batches // 2, turn, 0)

    def score(b):
        wide = jnp.concatenate([turned[b]] * (heads * head // LANES), axis=1) * mask[...]
        keys = kbuf[lax.rem(b, SLOTS)].reshape(heads * head, tokens)
        scores = jnp.dot(wide, keys, preferred_element_type=jnp.float32) * scale
        high = jnp.max(scores, 1, keepdims=True)
        w = jnp.exp(scores - high)
        total = jnp.sum(w, 1, keepdims=True)
        return w.astype(jnp.bfloat16), jnp.where(lane == head, high, jnp.where(lane == head + 1, total, 0.0))

    def keep(b, result):
        weights[lax.rem(b, 2)] = result[0]
        stats[lax.rem(b, 2)] = result[1]

    def gather_values(b):
        values = vbuf[lax.rem(b, SLOTS)].reshape(heads * head, tokens)
        every = lax.dot_general(values, weights[lax.rem(b, 2)], (((1,), (1,)), ((), ())),
                                preferred_element_type=jnp.float32)
        which = lax.broadcasted_iota(jnp.int32, (head, heads), 1)
        own = jnp.zeros((head, heads), jnp.float32)
        for h in range(heads):
            own = jnp.where(which == h, every[h * head:(h + 1) * head], own)
        return own

    def finish(b, own):
        send[b, :, :] = stats[lax.rem(b, 2)]
        send[b, :, :head] = own.T

    def scatter(b):
        chip = owner_chip(b)
        for core in range(2):
            target = 2 * chip + core

            @pl.when(target != me)
            def _():
                pltpu.make_async_remote_copy(
                    src_ref=send.at[b, pl.ds(core * half, half)],
                    dst_ref=recv.at[b // 8, lax.rem(me - target + 2 * n - 1, n)],
                    send_sem=rs_send, recv_sem=rs_recv.at[b // 8],
                    device_id={"sp": target}, device_id_type=pl.DeviceIdType.MESH,
                ).start()

    def combine(r):
        b = 8 * r + lax.rem(3 * my_chip + 4, 8)
        pltpu.make_async_copy(recv.at[r], recv.at[r], rs_recv.at[r]).wait()
        rows = pl.ds(pl.multiple_of(my_core * half, half), half)
        mine = send[b, rows, :]
        parts = [mine] + [recv[r, i] for i in range(n - 1)]
        highs = [p[:, head:head + 1] for p in parts]
        high = functools.reduce(jnp.maximum, highs)
        seen = jnp.zeros_like(mine)
        for p, h in zip(parts, highs):
            seen += p * jnp.exp(h - high)
        result = seen[:, :head] / seen[:, head + 1:head + 2]
        out_ref[b, rows, :] = result.astype(out_ref.dtype)
        for d in range(1, n):
            pltpu.make_async_remote_copy(
                src_ref=out_ref.at[b, rows], dst_ref=out_ref.at[b, rows],
                send_sem=ag_send, recv_sem=ag_recv,
                device_id={"sp": lax.rem(me + d, n)}, device_id_type=pl.DeviceIdType.MESH,
            ).start()

    fetch(k_hbm, kbuf, ksem, 0).wait()
    keep(0, score(0))
    pl.semaphore_wait(barrier, n - 1)

    def step(s, carry):
        b = s - 1
        fetch(k_hbm, kbuf, ksem, s).wait()
        fetch(v_hbm, vbuf, vsem, b).wait()
        result = score(s)
        own = gather_values(b)
        keep(s, result)
        finish(b, own)

        @pl.when(b + SLOTS < batches)
        def _():
            fetch(k_hbm, kbuf, ksem, b + SLOTS).start()
            fetch(v_hbm, vbuf, vsem, b + SLOTS).start()

        scatter(b)

        @pl.when((b >= 8) & (owner_chip(b) == my_chip))
        def _():
            combine(b // 8 - 1)

        return carry

    lax.fori_loop(1, batches, step, 0)
    last = batches - 1
    fetch(v_hbm, vbuf, vsem, last).wait()
    finish(last, gather_values(last))
    scatter(last)

    @pl.when(owner_chip(last) == my_chip)
    def _():
        combine(batches // 8 - 2)

    combine(batches // 8 - 1)
    pltpu.make_async_copy(recv, recv, rs_send).wait()
    sent = out_ref.at[pl.ds(0, batches // 16 * (n - 1))]
    pltpu.make_async_copy(sent, sent, ag_recv).wait()
    pltpu.make_async_copy(sent, sent, ag_send).wait()


def attend(q, k, v):
    batches, tokens, heads, head = k.shape
    n = 16
    return pl.pallas_call(
        functools.partial(kernel, head ** -0.5),
        out_shape=jax.ShapeDtypeStruct(q.shape, jnp.bfloat16),
        in_specs=[pl.BlockSpec(memory_space=pltpu.VMEM), pl.BlockSpec(memory_space=pl.ANY),
                  pl.BlockSpec(memory_space=pl.ANY)],
        out_specs=pl.BlockSpec(memory_space=pltpu.VMEM),
        scratch_shapes=[
            pltpu.VMEM((SLOTS, heads, head, tokens), jnp.bfloat16),
            pltpu.VMEM((SLOTS, heads, head, tokens), jnp.bfloat16),
            pltpu.VMEM((heads, heads * head), jnp.bfloat16),
            pltpu.VMEM((2, heads, LANES), jnp.float32),
            pltpu.VMEM((batches, heads, LANES), jnp.bfloat16),
            pltpu.VMEM((2, heads, tokens), jnp.bfloat16),
            pltpu.VMEM((2, heads, LANES), jnp.float32),
            pltpu.VMEM((batches, heads, LANES), jnp.float32),
            pltpu.VMEM((batches // 8, n - 1, heads // 2, LANES), jnp.float32),
            pltpu.SemaphoreType.DMA((SLOTS,)),
            pltpu.SemaphoreType.DMA((SLOTS,)),
            pltpu.SemaphoreType.DMA,
            pltpu.SemaphoreType.DMA((batches // 8,)),
            pltpu.SemaphoreType.DMA,
            pltpu.SemaphoreType.DMA,
        ],
        compiler_params=pltpu.CompilerParams(collective_id=0, has_side_effects=True, vmem_limit_bytes=60 * 2**20),
    )(q, jnp.transpose(k, (0, 2, 3, 1)), jnp.transpose(v, (0, 2, 3, 1)))


def solution(mesh):
    return jax.shard_map(
        attend,
        mesh=mesh,
        in_specs=(P("dp", None, None), P("dp", "sp", None, None), P("dp", "sp", None, None)),
        out_specs=P("dp", None, None),
        check_vma=False,
    )
```

```python
import functools

import jax
import jax.numpy as jnp
from jax import lax
from jax.experimental import pallas as pl
from jax.experimental.pallas import tpu as pltpu
from jax.sharding import PartitionSpec as P

SLOTS = 8
LAG = 5
LANES = 128
N = 16
GROUPS = 2


def chip_of(i):
    inner, t = i // 4, lax.rem(i, 2)
    return lax.rem(i, 4) // 2 * 4 + inner * (1 + t) + (1 - inner) * 3 * t


def batch_of(chip):
    y, z = chip // 4, lax.rem(chip, 4)
    inner = z * (3 - z) // 2
    return 4 * inner + 2 * y + inner * (z - 1) + (1 - inner) * (z // 3)


def kernel(scale, q_hbm, k_hbm, v_hbm, out_ref, q_ref, kbuf, vbuf, mask, qpad, turned, weights, stats, send, recv,
           qsem, ksem, vsem, part_send_sem, part_sem, out_send_sem, out_sem):
    batches, heads, head = q_ref.shape
    tokens = k_hbm.shape[-1]
    half = heads // 2
    run = heads // GROUPS
    rounds = batches // 8
    me = lax.axis_index("sp")
    my_batch, my_core = batch_of(me // 2), lax.rem(me, 2)

    def fetch(hbm, buf, sem, b):
        return pltpu.make_async_copy(hbm.at[b], buf.at[lax.rem(b, SLOTS)], sem.at[lax.rem(b, SLOTS)])

    def give(src, dst, send_sem, recv_sem, target):
        return pltpu.make_async_remote_copy(src_ref=src, dst_ref=dst, send_sem=send_sem, recv_sem=recv_sem,
                                            device_id={"sp": target}, device_id_type=pl.DeviceIdType.MESH)

    q_copy = pltpu.make_async_copy(q_hbm, q_ref, qsem)
    fetch(k_hbm, kbuf, ksem, 0).start()
    q_copy.start()
    for b in range(SLOTS):
        if b:
            fetch(k_hbm, kbuf, ksem, b).start(priority=1)
        fetch(v_hbm, vbuf, vsem, b).start(priority=1)

    barrier = pltpu.get_barrier_semaphore()
    for d in range(1, N):
        pl.semaphore_signal(barrier, 1, device_id={"sp": lax.rem(me + d, N)}, device_id_type=pl.DeviceIdType.MESH)

    row = lax.broadcasted_iota(jnp.int32, (run, run * head), 0) * head
    col = lax.broadcasted_iota(jnp.int32, (run, run * head), 1)
    mask[...] = jnp.where((col >= row) & (col < row + head), 1.0, 0.0).astype(jnp.bfloat16)
    qpad[...] = jnp.zeros_like(qpad)
    lane = lax.broadcasted_iota(jnp.int32, (run, LANES), 1)
    which = lax.broadcasted_iota(jnp.int32, (head, run), 1)
    shift = lax.rem(lax.broadcasted_iota(jnp.int32, (heads, LANES), 0) * head, LANES)

    def turn(b, i):
        qpad[i, :, :head] = q_ref[jnp.minimum(b, batches - 1)].astype(jnp.float32)
        x = qpad[i]
        for bit in (16, 32, 64):
            x = jnp.where((shift & bit) != 0, pltpu.roll(x, bit, 1), x)
        turned[i] = x.astype(jnp.bfloat16)

    def score(b, queries):
        weights, stats = [], []
        for g in range(GROUPS):
            wide = jnp.concatenate([queries[g * run:(g + 1) * run]] * (run * head // LANES), axis=1) * mask[...]
            keys = kbuf[lax.rem(b, SLOTS), g * run:(g + 1) * run].reshape(run * head, tokens)
            scores = jnp.dot(wide, keys, preferred_element_type=jnp.float32) * scale
            high = jnp.max(scores, 1, keepdims=True)
            w = jnp.exp(scores - high)
            total = jnp.sum(w, 1, keepdims=True)
            weights.append(w.astype(jnp.bfloat16))
            stats.append(jnp.where(lane == head, high, jnp.where(lane == head + 1, total, 0.0)))
        return weights, stats

    def see(b, weights):
        sums = []
        for g in range(GROUPS):
            values = vbuf[lax.rem(b, SLOTS), g * run:(g + 1) * run].reshape(run * head, tokens)
            every = lax.dot_general(values, weights[g], (((1,), (1,)), ((), ())), preferred_element_type=jnp.float32)
            own = jnp.zeros((head, run), jnp.float32)
            for h in range(run):
                own = jnp.where(which == h, every[h * head:(h + 1) * head], own)
            sums.append(own.T)
        return sums

    def part(b, sums, stats):
        for g in range(GROUPS):
            send[b, g * run:(g + 1) * run, :] = stats[g]
            send[b, g * run:(g + 1) * run, :head] = sums[g]

    def keep(new):
        for g in range(GROUPS):
            weights[g], stats[g] = new[0][g], new[1][g]

    def kept():
        return [weights[g] for g in range(GROUPS)], [stats[g] for g in range(GROUPS)]

    def scatter(b):
        for core in range(2):
            target = 2 * chip_of(lax.rem(b, 8)) + core

            @pl.when(target != me)
            def _():
                give(send.at[b, pl.ds(core * half, half)], recv.at[b // 8, lax.rem(me - target + 2 * N - 1, N)],
                     part_send_sem, part_sem.at[b // 8], target).start()

    def combine(r):
        b = 8 * r + my_batch
        pltpu.make_async_copy(recv.at[r], recv.at[r], part_sem.at[r]).wait()
        rows = pl.ds(pl.multiple_of(my_core * half, half), half)
        parts = [send[b, rows, :]] + [recv[r, i] for i in range(N - 1)]
        highs = [p[:, head:head + 1] for p in parts]
        high = functools.reduce(jnp.maximum, highs)
        seen = functools.reduce(jnp.add, [p * jnp.exp(h - high) for p, h in zip(parts, highs)])
        out_ref[b, rows, :] = (seen[:, :head] / seen[:, head + 1:head + 2]).astype(out_ref.dtype)
        for d in range(1, N):
            give(out_ref.at[b, rows], out_ref.at[b, rows], out_send_sem, out_sem, lax.rem(me + d, N)).start()

    q_copy.wait()
    turn(0, 0)
    first = turned[0]
    turn(1, 0)
    turn(2, 1)
    fetch(k_hbm, kbuf, ksem, 0).wait()
    keep(score(0, first))

    def step(i, carry):
        b = 2 * i
        fetch(k_hbm, kbuf, ksem, b + 1).wait()
        fetch(v_hbm, vbuf, vsem, b).wait()
        fetch(k_hbm, kbuf, ksem, b + 2).wait()
        fetch(v_hbm, vbuf, vsem, b + 1).wait()
        w0, s0 = kept()
        queries = [turned[0], turned[1]]
        w1, s1 = score(b + 1, queries[0])
        r0 = see(b, w0)
        new = score(b + 2, queries[1])
        r1 = see(b + 1, w1)
        turn(b + 3, 0)
        turn(b + 4, 1)
        part(b, r0, s0)
        part(b + 1, r1, s1)
        keep(new)

        for j in range(2):
            @pl.when(b + j + 1 + SLOTS < batches)
            def _():
                fetch(k_hbm, kbuf, ksem, b + j + 1 + SLOTS).start(priority=1)

            @pl.when(b + j + SLOTS < batches)
            def _():
                fetch(v_hbm, vbuf, vsem, b + j + SLOTS).start(priority=1)

        @pl.when(i == 0)
        def _():
            pl.semaphore_wait(barrier, N - 1)

        scatter(b)
        scatter(b + 1)

        for j in range(2):
            @pl.when((i >= LAG) & (lax.rem(b + j - 2 * LAG + 8, 8) == my_batch))
            def _():
                combine((b + j - 2 * LAG) // 8)

        return carry

    fetch(k_hbm, kbuf, ksem, SLOTS).start()
    lax.fori_loop(0, batches // 2 - 1, step, 0)
    last = batches - 1
    fetch(k_hbm, kbuf, ksem, last).wait()
    fetch(v_hbm, vbuf, vsem, last - 1).wait()
    w0, s0 = kept()
    w1, s1 = score(last, turned[0])
    part(last - 1, see(last - 1, w0), s0)
    scatter(last - 1)
    fetch(v_hbm, vbuf, vsem, last).wait()
    part(last, see(last, w1), s1)
    scatter(last)

    @pl.when(batches - 16 + my_batch >= batches - 2 * LAG - 2)
    def _():
        combine(rounds - 2)

    combine(rounds - 1)

    pltpu.make_async_copy(recv, recv, part_send_sem).wait()
    sent = out_ref.at[pl.ds(0, rounds * (N - 1) // 2)]
    pltpu.make_async_copy(sent, sent, out_sem).wait()
    pltpu.make_async_copy(sent, sent, out_send_sem).wait()


def attend(q, k, v):
    batches, tokens, heads, head = k.shape
    run = heads // GROUPS
    return pl.pallas_call(
        functools.partial(kernel, head ** -0.5),
        out_shape=jax.ShapeDtypeStruct(q.shape, jnp.bfloat16),
        in_specs=[pl.BlockSpec(memory_space=pltpu.HBM)] * 3,
        out_specs=pl.BlockSpec(memory_space=pltpu.VMEM),
        scratch_shapes=[
            pltpu.VMEM(q.shape, jnp.bfloat16),
            pltpu.VMEM((SLOTS, heads, head, tokens), jnp.bfloat16),
            pltpu.VMEM((SLOTS, heads, head, tokens), jnp.bfloat16),
            pltpu.VMEM((run, run * head), jnp.bfloat16),
            pltpu.VMEM((2, heads, LANES), jnp.float32),
            pltpu.VMEM((2, heads, LANES), jnp.bfloat16),
            pltpu.VMEM((GROUPS, run, tokens), jnp.bfloat16),
            pltpu.VMEM((GROUPS, run, LANES), jnp.float32),
            pltpu.VMEM((batches, heads, LANES), jnp.float32),
            pltpu.VMEM((batches // 8, N - 1, heads // 2, LANES), jnp.float32),
            pltpu.SemaphoreType.DMA,
            pltpu.SemaphoreType.DMA((SLOTS,)),
            pltpu.SemaphoreType.DMA((SLOTS,)),
            pltpu.SemaphoreType.DMA,
            pltpu.SemaphoreType.DMA((batches // 8,)),
            pltpu.SemaphoreType.DMA,
            pltpu.SemaphoreType.DMA,
        ],
        compiler_params=pltpu.CompilerParams(collective_id=0, has_side_effects=True, vmem_limit_bytes=30 * 2**20),
    )(pltpu.with_memory_space_constraint(q, pltpu.HBM), jnp.transpose(k, (0, 2, 3, 1)), jnp.transpose(v, (0, 2, 3, 1)))


def solution(mesh):
    return jax.shard_map(
        attend,
        mesh=mesh,
        in_specs=(P("dp", None, None), P("dp", "sp", None, None), P("dp", "sp", None, None)),
        out_specs=P("dp", None, None),
        check_vma=False,
    )
```

```python
import functools

import jax
import jax.numpy as jnp
from jax import lax
from jax.experimental import pallas as pl
from jax.experimental.pallas import tpu as pltpu
from jax.sharding import PartitionSpec as P

SLOTS = 8
LAG = 4
LANES = 128
N = 16
GROUPS = 2
TAIL = 2


def owner_of(b, half):
    high, low = lax.rem(b, 4) // 2, lax.rem(b, 2)
    z = (1 - high) * (3 - low) + high * low
    return (4 * half + z) * 2 + lax.rem(b // 4, 2)


def batch_of(device):
    z, core = lax.rem(device // 2, 4), lax.rem(device, 2)
    back = z // 2
    return 4 * core + 2 * (1 - back) + back * (3 - z) + (1 - back) * z


def kernel(scale, q_hbm, k_hbm, v_hbm, out_ref, q_ref, kbuf, vbuf, mask, qpad, turned, weights, stats, send, recv,
           qsem, ksem, vsem, part_send_sem, part_sem, out_send_sem, out_sem):
    batches, heads, head = q_ref.shape
    tokens = k_hbm.shape[-1]
    half = heads // 2
    run = heads // GROUPS
    rounds = batches // 8
    me = lax.axis_index("sp")
    my_batch = batch_of(me)
    mine = pl.ds(pl.multiple_of(me // 8 * half, half), half)

    def fetch(hbm, buf, sem, b):
        return pltpu.make_async_copy(hbm.at[b], buf.at[lax.rem(b, SLOTS)], sem.at[lax.rem(b, SLOTS)])

    def give(src, dst, send_sem, recv_sem, target):
        return pltpu.make_async_remote_copy(src_ref=src, dst_ref=dst, send_sem=send_sem, recv_sem=recv_sem,
                                            device_id={"sp": target}, device_id_type=pl.DeviceIdType.MESH)

    q_copy = pltpu.make_async_copy(q_hbm, q_ref, qsem)
    fetch(k_hbm, kbuf, ksem, 0).start()
    q_copy.start()
    for b in range(SLOTS):
        if b:
            fetch(k_hbm, kbuf, ksem, b).start(priority=1)
        fetch(v_hbm, vbuf, vsem, b).start(priority=1)

    barrier = pltpu.get_barrier_semaphore()
    for d in range(1, N):
        pl.semaphore_signal(barrier, 1, device_id={"sp": lax.rem(me + d, N)}, device_id_type=pl.DeviceIdType.MESH)

    row = lax.broadcasted_iota(jnp.int32, (run, run * head), 0) * head
    col = lax.broadcasted_iota(jnp.int32, (run, run * head), 1)
    mask[...] = jnp.where((col >= row) & (col < row + head), 1.0, 0.0).astype(jnp.bfloat16)
    qpad[...] = jnp.zeros_like(qpad)
    lane = lax.broadcasted_iota(jnp.int32, (run, LANES), 1)
    which = lax.broadcasted_iota(jnp.int32, (head, run), 1)
    shift = lax.rem(lax.broadcasted_iota(jnp.int32, (heads, LANES), 0) * head, LANES)

    def turn(b, i):
        qpad[i, :, :head] = q_ref[jnp.minimum(b, batches - 1)].astype(jnp.float32)
        x = qpad[i]
        for bit in (16, 32, 64):
            x = jnp.where((shift & bit) != 0, pltpu.roll(x, bit, 1), x)
        turned[i] = x.astype(jnp.bfloat16)

    def score(b, queries):
        weights, stats = [], []
        for g in range(GROUPS):
            wide = jnp.concatenate([queries[g * run:(g + 1) * run]] * (run * head // LANES), axis=1) * mask[...]
            keys = kbuf[lax.rem(b, SLOTS), g * run:(g + 1) * run].reshape(run * head, tokens)
            scores = jnp.dot(wide, keys, preferred_element_type=jnp.float32) * scale
            high = jnp.max(scores, 1, keepdims=True)
            w = jnp.exp(scores - high)
            total = jnp.sum(w, 1, keepdims=True)
            weights.append(w.astype(jnp.bfloat16))
            stats.append(jnp.where(lane == head, high, jnp.where(lane == head + 1, total, 0.0)))
        return weights, stats

    def see(b, weights):
        sums = []
        for g in range(GROUPS):
            values = vbuf[lax.rem(b, SLOTS), g * run:(g + 1) * run].reshape(run * head, tokens)
            every = lax.dot_general(values, weights[g], (((1,), (1,)), ((), ())), preferred_element_type=jnp.float32)
            own = jnp.zeros((head, run), jnp.float32)
            for h in range(run):
                own = jnp.where(which == h, every[h * head:(h + 1) * head], own)
            sums.append(own.T)
        return sums

    def part(b, sums, stats):
        for g in range(GROUPS):
            send[b, g * run:(g + 1) * run, :] = stats[g]
            send[b, g * run:(g + 1) * run, :head] = sums[g]

    def keep(i, new):
        for g in range(GROUPS):
            weights[i, g], stats[i, g] = new[0][g], new[1][g]

    def kept(i):
        return [weights[i, g] for g in range(GROUPS)], [stats[i, g] for g in range(GROUPS)]

    def scatter(b):
        for h in range(2):
            target = owner_of(b, h)

            @pl.when(target != me)
            def _():
                give(send.at[b, pl.ds(h * half, half)], recv.at[b // 8, lax.rem(me - target + 2 * N - 1, N)],
                     part_send_sem, part_sem.at[b // 8], target).start()

    def combine(r):
        b = 8 * r + my_batch
        pltpu.make_async_copy(recv.at[r], recv.at[r], part_sem.at[r]).wait()
        parts = [send[b, mine, :]] + [recv[r, i] for i in range(N - 1)]
        highs = [p[:, head:head + 1] for p in parts]
        high = functools.reduce(jnp.maximum, highs)
        seen = functools.reduce(jnp.add, [p * jnp.exp(h - high) for p, h in zip(parts, highs)])
        out_ref[b, mine, :] = (seen[:, :head] / seen[:, head + 1:head + 2]).astype(out_ref.dtype)
        for d in range(1, N):
            give(out_ref.at[b, mine], out_ref.at[b, mine], out_send_sem, out_sem, lax.rem(me + d, N)).start()

    q_copy.wait()
    turn(0, 0)
    turn(1, 1)
    for b in range(2):
        fetch(k_hbm, kbuf, ksem, b).wait()
    queries = [turned[0], turned[1]]
    turn(2, 0)
    turn(3, 1)
    for b in range(2):
        keep(b, score(b, queries[b]))
    for b in range(2):
        fetch(k_hbm, kbuf, ksem, SLOTS + b).start(priority=1)

    def work(b, count):
        for j in range(count):
            fetch(k_hbm, kbuf, ksem, b + 2 + j).wait()
            fetch(v_hbm, vbuf, vsem, b + j).wait()
        slots = [lax.rem(b + j, 2) for j in range(count)]
        old = [kept(i) for i in slots]
        queries = [turned[i] for i in slots]
        new, sums = [], []
        for j in range(count):
            new.append(score(b + 2 + j, queries[j]))
            sums.append(see(b + j, old[j][0]))
        for j in range(count):
            turn(b + 4 + j, slots[j])
            part(b + j, sums[j], old[j][1])
            keep(slots[j], new[j])

    def exchange(b, count):
        for j in range(count):
            scatter(b + j)
        for j in range(count):
            @pl.when((b >= 2 * LAG) & (lax.rem(b + j - 2 * LAG + 8, 8) == my_batch))
            def _():
                combine((b + j - 2 * LAG) // 8)

    def step(i, carry):
        b = 2 * i
        work(b, 2)

        @pl.when(b + 2 + SLOTS < batches)
        def _():
            for j in range(2):
                fetch(k_hbm, kbuf, ksem, b + 2 + j + SLOTS).start(priority=1)
                fetch(v_hbm, vbuf, vsem, b + j + SLOTS).start(priority=1)

        @pl.when(b + 2 + SLOTS == batches)
        def _():
            for j in range(2):
                fetch(v_hbm, vbuf, vsem, b + j + SLOTS).start(priority=1)

        @pl.when(i == 0)
        def _():
            pl.semaphore_wait(barrier, N - 1)

        exchange(b, 2)
        return carry

    def single(b, carry):
        work(b, 1)
        exchange(b, 1)
        return carry

    lax.fori_loop(0, (batches - SLOTS) // 2, step, 0)
    lax.fori_loop(batches - SLOTS, batches - TAIL, single, 0)

    for b in range(batches - TAIL, batches):
        w, st = kept(b % 2)
        fetch(v_hbm, vbuf, vsem, b).wait()
        part(b, see(b, w), st)
        scatter(b)

    @pl.when(my_batch >= 8 - 2 * LAG + 8 - TAIL)
    def _():
        combine(rounds - 2)

    combine(rounds - 1)

    pltpu.make_async_copy(recv, recv, part_send_sem).wait()
    sent = out_ref.at[pl.ds(0, rounds * (N - 1) // 2)]
    pltpu.make_async_copy(sent, sent, out_sem).wait()
    pltpu.make_async_copy(sent, sent, out_send_sem).wait()


def attend(q, k, v):
    batches, tokens, heads, head = k.shape
    run = heads // GROUPS
    return pl.pallas_call(
        functools.partial(kernel, head ** -0.5),
        out_shape=jax.ShapeDtypeStruct(q.shape, jnp.bfloat16),
        in_specs=[pl.BlockSpec(memory_space=pltpu.HBM)] * 3,
        out_specs=pl.BlockSpec(memory_space=pltpu.VMEM),
        scratch_shapes=[
            pltpu.VMEM(q.shape, jnp.bfloat16),
            pltpu.VMEM((SLOTS, heads, head, tokens), jnp.bfloat16),
            pltpu.VMEM((SLOTS, heads, head, tokens), jnp.bfloat16),
            pltpu.VMEM((run, run * head), jnp.bfloat16),
            pltpu.VMEM((2, heads, LANES), jnp.float32),
            pltpu.VMEM((2, heads, LANES), jnp.bfloat16),
            pltpu.VMEM((2, GROUPS, run, tokens), jnp.bfloat16),
            pltpu.VMEM((2, GROUPS, run, LANES), jnp.float32),
            pltpu.VMEM((batches, heads, LANES), jnp.float32),
            pltpu.VMEM((batches // 8, N - 1, heads // 2, LANES), jnp.float32),
            pltpu.SemaphoreType.DMA,
            pltpu.SemaphoreType.DMA((SLOTS,)),
            pltpu.SemaphoreType.DMA((SLOTS,)),
            pltpu.SemaphoreType.DMA,
            pltpu.SemaphoreType.DMA((batches // 8,)),
            pltpu.SemaphoreType.DMA,
            pltpu.SemaphoreType.DMA,
        ],
        compiler_params=pltpu.CompilerParams(collective_id=0, has_side_effects=True, vmem_limit_bytes=30 * 2**20),
    )(pltpu.with_memory_space_constraint(q, pltpu.HBM), jnp.transpose(k, (0, 2, 3, 1)), jnp.transpose(v, (0, 2, 3, 1)))


def solution(mesh):
    return jax.shard_map(
        attend,
        mesh=mesh,
        in_specs=(P("dp", None, None), P("dp", "sp", None, None), P("dp", "sp", None, None)),
        out_specs=P("dp", None, None),
        check_vma=False,
    )
```

```python
import functools

import jax
import jax.numpy as jnp
from jax import lax
from jax.experimental import pallas as pl
from jax.experimental.pallas import tpu as pltpu
from jax.sharding import PartitionSpec as P

SLOTS = 8
LAG = 4
LANES = 128
N = 16
GROUPS = 2
TAIL = 2


def owner_of(b, half):
    high, low = lax.rem(b, 4) // 2, lax.rem(b, 2)
    z = (1 - high) * (3 - low) + high * low
    return (4 * half + z) * 2 + lax.rem(b // 4, 2)


def batch_of(device):
    z, core = lax.rem(device // 2, 4), lax.rem(device, 2)
    back = z // 2
    return 4 * core + 2 * (1 - back) + back * (3 - z) + (1 - back) * z


def kernel(scale, q_hbm, k_hbm, v_hbm, out_ref, q_ref, kbuf, vbuf, mask, qpad, turned, weights, stats, send, recv,
           qsem, ksem, vsem, part_send_sem, part_sem, out_send_sem, out_sem):
    batches, heads, head = q_ref.shape
    tokens = k_hbm.shape[-1]
    half = heads // 2
    run = heads // GROUPS
    rounds = batches // 8
    me = lax.axis_index("sp")
    my_batch = batch_of(me)
    mine = pl.ds(pl.multiple_of(me // 8 * half, half), half)

    def fetch(hbm, buf, sem, b):
        return pltpu.make_async_copy(hbm.at[b], buf.at[lax.rem(b, SLOTS)], sem.at[lax.rem(b, SLOTS)])

    def give(src, dst, send_sem, recv_sem, target):
        return pltpu.make_async_remote_copy(src_ref=src, dst_ref=dst, send_sem=send_sem, recv_sem=recv_sem,
                                            device_id={"sp": target}, device_id_type=pl.DeviceIdType.MESH)

    q_copy = pltpu.make_async_copy(q_hbm, q_ref, qsem)
    fetch(k_hbm, kbuf, ksem, 0).start()
    q_copy.start()
    for b in range(SLOTS):
        if b:
            fetch(k_hbm, kbuf, ksem, b).start(priority=1)
        fetch(v_hbm, vbuf, vsem, b).start(priority=1)

    barrier = pltpu.get_barrier_semaphore()
    for d in range(1, N):
        pl.semaphore_signal(barrier, 1, device_id={"sp": lax.rem(me + d, N)}, device_id_type=pl.DeviceIdType.MESH)

    row = lax.broadcasted_iota(jnp.int32, (run, run * head), 0) * head
    col = lax.broadcasted_iota(jnp.int32, (run, run * head), 1)
    mask[...] = jnp.where((col >= row) & (col < row + head), 1.0, 0.0).astype(jnp.bfloat16)
    qpad[...] = jnp.zeros_like(qpad)
    lane = lax.broadcasted_iota(jnp.int32, (run, LANES), 1)
    which = lax.broadcasted_iota(jnp.int32, (head, run), 1)
    shift = lax.rem(lax.broadcasted_iota(jnp.int32, (heads, LANES), 0) * head, LANES)

    def turn(b, i):
        qpad[i, :, :head] = q_ref[jnp.minimum(b, batches - 1)].astype(jnp.float32)
        x = qpad[i]
        for bit in (16, 32, 64):
            x = jnp.where((shift & bit) != 0, pltpu.roll(x, bit, 1), x)
        turned[i] = x.astype(jnp.bfloat16)

    def score(b, queries):
        weights, stats = [], []
        for g in range(GROUPS):
            wide = jnp.concatenate([queries[g * run:(g + 1) * run]] * (run * head // LANES), axis=1) * mask[...]
            keys = kbuf[lax.rem(b, SLOTS), g * run:(g + 1) * run].reshape(run * head, tokens)
            scores = jnp.dot(wide, keys, preferred_element_type=jnp.float32) * scale
            high = jnp.max(scores, 1, keepdims=True)
            w = jnp.exp(scores - high)
            total = jnp.sum(w, 1, keepdims=True)
            weights.append(w.astype(jnp.bfloat16))
            stats.append(jnp.where(lane == head, high, jnp.where(lane == head + 1, total, 0.0)))
        return weights, stats

    def see(b, weights):
        sums = []
        for g in range(GROUPS):
            values = vbuf[lax.rem(b, SLOTS), g * run:(g + 1) * run].reshape(run * head, tokens)
            every = lax.dot_general(values, weights[g], (((1,), (1,)), ((), ())), preferred_element_type=jnp.float32)
            own = jnp.zeros((head, run), jnp.float32)
            for h in range(run):
                own = jnp.where(which == h, every[h * head:(h + 1) * head], own)
            sums.append(own.T)
        return sums

    def part(b, sums, stats):
        for g in range(GROUPS):
            send[b, g * run:(g + 1) * run, :] = stats[g]
            send[b, g * run:(g + 1) * run, :head] = sums[g]

    def keep(i, new):
        for g in range(GROUPS):
            weights[i, g], stats[i, g] = new[0][g], new[1][g]

    def kept(i):
        return [weights[i, g] for g in range(GROUPS)], [stats[i, g] for g in range(GROUPS)]

    def scatter(b):
        for h in range(2):
            target = owner_of(b, h)

            @pl.when(target != me)
            def _():
                give(send.at[b, pl.ds(h * half, half)], recv.at[b // 8, lax.rem(me - target + 2 * N - 1, N)],
                     part_send_sem, part_sem.at[b // 8], target).start()

    def combine(r):
        b = 8 * r + my_batch
        pltpu.make_async_copy(recv.at[r], recv.at[r], part_sem.at[r]).wait()
        parts = [send[b, mine, :]] + [recv[r, i] for i in range(N - 1)]
        highs = [p[:, head:head + 1] for p in parts]
        high = functools.reduce(jnp.maximum, highs)
        seen = functools.reduce(jnp.add, [p * jnp.exp(h - high) for p, h in zip(parts, highs)])
        out_ref[b, mine, :] = (seen[:, :head] / seen[:, head + 1:head + 2]).astype(out_ref.dtype)
        for d in range(1, N):
            give(out_ref.at[b, mine], out_ref.at[b, mine], out_send_sem, out_sem, lax.rem(me + d, N)).start()

    q_copy.wait()
    turn(0, 0)
    turn(1, 1)
    for b in range(2):
        fetch(k_hbm, kbuf, ksem, b).wait()
    queries = [turned[0], turned[1]]
    turn(2, 0)
    turn(3, 1)
    for b in range(2):
        keep(b, score(b, queries[b]))
    for b in range(2):
        fetch(k_hbm, kbuf, ksem, SLOTS + b).start(priority=1)

    def work(b, count):
        for j in range(count):
            fetch(k_hbm, kbuf, ksem, b + 2 + j).wait()
            fetch(v_hbm, vbuf, vsem, b + j).wait()
        slots = [lax.rem(b + j, 2) for j in range(count)]
        old = [kept(i) for i in slots]
        queries = [turned[i] for i in slots]
        new, sums = [], []
        for j in range(count):
            new.append(score(b + 2 + j, queries[j]))
            sums.append(see(b + j, old[j][0]))
        for j in range(count):
            turn(b + 4 + j, slots[j])
            part(b + j, sums[j], old[j][1])
            keep(slots[j], new[j])

    def exchange(b, count):
        for j in range(count):
            scatter(b + j)
        for j in range(count):
            @pl.when((b >= 2 * LAG) & (lax.rem(b + j - 2 * LAG + 8, 8) == my_batch))
            def _():
                combine((b + j - 2 * LAG) // 8)

    def step(i, carry):
        b = 2 * i
        work(b, 2)

        @pl.when(b + 2 + SLOTS < batches)
        def _():
            for j in range(2):
                fetch(k_hbm, kbuf, ksem, b + 2 + j + SLOTS).start(priority=1)
                fetch(v_hbm, vbuf, vsem, b + j + SLOTS).start(priority=1)

        @pl.when(b + 2 + SLOTS == batches)
        def _():
            for j in range(2):
                fetch(v_hbm, vbuf, vsem, b + j + SLOTS).start(priority=1)

        @pl.when(i == 0)
        def _():
            pl.semaphore_wait(barrier, N - 1)

        exchange(b, 2)
        return carry

    def single(b, carry):
        work(b, 1)
        exchange(b, 1)
        return carry

    lax.fori_loop(0, (batches - 4) // 2, step, 0)
    lax.fori_loop(batches - 4, batches - TAIL, single, 0)

    for b in range(batches - TAIL, batches):
        w, st = kept(b % 2)
        fetch(v_hbm, vbuf, vsem, b).wait()
        part(b, see(b, w), st)
        scatter(b)

    @pl.when(my_batch >= 8 - 2 * LAG + 8 - TAIL)
    def _():
        combine(rounds - 2)

    combine(rounds - 1)

    pltpu.make_async_copy(recv, recv, part_send_sem).wait()
    sent = out_ref.at[pl.ds(0, rounds * (N - 1) // 2)]
    pltpu.make_async_copy(sent, sent, out_sem).wait()
    pltpu.make_async_copy(sent, sent, out_send_sem).wait()


def attend(q, k, v):
    batches, tokens, heads, head = k.shape
    run = heads // GROUPS
    return pl.pallas_call(
        functools.partial(kernel, head ** -0.5),
        out_shape=jax.ShapeDtypeStruct(q.shape, jnp.bfloat16),
        in_specs=[pl.BlockSpec(memory_space=pltpu.HBM)] * 3,
        out_specs=pl.BlockSpec(memory_space=pltpu.VMEM),
        scratch_shapes=[
            pltpu.VMEM(q.shape, jnp.bfloat16),
            pltpu.VMEM((SLOTS, heads, head, tokens), jnp.bfloat16),
            pltpu.VMEM((SLOTS, heads, head, tokens), jnp.bfloat16),
            pltpu.VMEM((run, run * head), jnp.bfloat16),
            pltpu.VMEM((2, heads, LANES), jnp.float32),
            pltpu.VMEM((2, heads, LANES), jnp.bfloat16),
            pltpu.VMEM((2, GROUPS, run, tokens), jnp.bfloat16),
            pltpu.VMEM((2, GROUPS, run, LANES), jnp.float32),
            pltpu.VMEM((batches, heads, LANES), jnp.float32),
            pltpu.VMEM((batches // 8, N - 1, heads // 2, LANES), jnp.float32),
            pltpu.SemaphoreType.DMA,
            pltpu.SemaphoreType.DMA((SLOTS,)),
            pltpu.SemaphoreType.DMA((SLOTS,)),
            pltpu.SemaphoreType.DMA,
            pltpu.SemaphoreType.DMA((batches // 8,)),
            pltpu.SemaphoreType.DMA,
            pltpu.SemaphoreType.DMA,
        ],
        compiler_params=pltpu.CompilerParams(collective_id=0, has_side_effects=True, vmem_limit_bytes=30 * 2**20),
    )(pltpu.with_memory_space_constraint(q, pltpu.HBM), jnp.transpose(k, (0, 2, 3, 1)), jnp.transpose(v, (0, 2, 3, 1)))


def solution(mesh):
    return jax.shard_map(
        attend,
        mesh=mesh,
        in_specs=(P("dp", None, None), P("dp", "sp", None, None), P("dp", "sp", None, None)),
        out_specs=P("dp", None, None),
        check_vma=False,
    )
```

```python
import functools

import jax
import jax.numpy as jnp
from jax import lax
from jax.experimental import pallas as pl
from jax.experimental.pallas import tpu as pltpu
from jax.sharding import PartitionSpec as P

SLOTS = 8
LAG = 4
LANES = 128
N = 16
GROUPS = 2
TAIL = 2


def owner_of(b, half):
    high, low = lax.rem(b, 4) // 2, lax.rem(b, 2)
    z = (1 - high) * (3 - low) + high * low
    return (4 * half + z) * 2 + lax.rem(b // 4, 2)


def batch_of(device):
    z, core = lax.rem(device // 2, 4), lax.rem(device, 2)
    back = z // 2
    return 4 * core + 2 * (1 - back) + back * (3 - z) + (1 - back) * z


def kernel(scale, q_hbm, k_hbm, v_hbm, out_ref, q_ref, kbuf, vbuf, mask, qpad, turned, weights, stats, send, recv,
           qsem, ksem, vsem, part_send_sem, part_sem, out_send_sem, out_sem):
    batches, heads, head = q_ref.shape
    tokens = k_hbm.shape[-1]
    half = heads // 2
    run = heads // GROUPS
    rounds = batches // 8
    me = lax.axis_index("sp")
    my_batch = batch_of(me)
    mine = pl.ds(pl.multiple_of(me // 8 * half, half), half)

    def fetch(hbm, buf, sem, b):
        return pltpu.make_async_copy(hbm.at[b], buf.at[lax.rem(b, SLOTS)], sem.at[lax.rem(b, SLOTS)])

    def give(src, dst, send_sem, recv_sem, target):
        return pltpu.make_async_remote_copy(src_ref=src, dst_ref=dst, send_sem=send_sem, recv_sem=recv_sem,
                                            device_id={"sp": target}, device_id_type=pl.DeviceIdType.MESH)

    q_copy = pltpu.make_async_copy(q_hbm, q_ref, qsem)
    fetch(k_hbm, kbuf, ksem, 0).start()
    q_copy.start()
    for b in range(SLOTS):
        if b:
            fetch(k_hbm, kbuf, ksem, b).start(priority=1)
        fetch(v_hbm, vbuf, vsem, b).start(priority=1)

    barrier = pltpu.get_barrier_semaphore()
    for d in range(1, N):
        pl.semaphore_signal(barrier, 1, device_id={"sp": lax.rem(me + d, N)}, device_id_type=pl.DeviceIdType.MESH)

    row = lax.broadcasted_iota(jnp.int32, (run, run * head), 0) * head
    col = lax.broadcasted_iota(jnp.int32, (run, run * head), 1)
    mask[...] = jnp.where((col >= row) & (col < row + head), 1.0, 0.0).astype(jnp.bfloat16)
    qpad[...] = jnp.zeros_like(qpad)
    lane = lax.broadcasted_iota(jnp.int32, (run, LANES), 1)
    which = lax.broadcasted_iota(jnp.int32, (head, run), 1)
    shift = lax.rem(lax.broadcasted_iota(jnp.int32, (heads, LANES), 0) * head, LANES)

    def turn(b, i):
        qpad[i, :, :head] = q_ref[jnp.minimum(b, batches - 1)].astype(jnp.float32)
        x = qpad[i]
        for bit in (16, 32, 64):
            x = jnp.where((shift & bit) != 0, pltpu.roll(x, bit, 1), x)
        turned[i] = x.astype(jnp.bfloat16)

    def score(b, queries):
        weights, stats = [], []
        for g in range(GROUPS):
            wide = jnp.concatenate([queries[g * run:(g + 1) * run]] * (run * head // LANES), axis=1) * mask[...]
            keys = kbuf[lax.rem(b, SLOTS), g * run:(g + 1) * run].reshape(run * head, tokens)
            scores = jnp.dot(wide, keys, preferred_element_type=jnp.float32) * scale
            high = jnp.max(scores, 1, keepdims=True)
            w = jnp.exp(scores - high)
            total = jnp.sum(w, 1, keepdims=True)
            weights.append(w.astype(jnp.bfloat16))
            stats.append(jnp.where(lane == head, high, jnp.where(lane == head + 1, total, 0.0)))
        return weights, stats

    def see(b, weights):
        sums = []
        for g in range(GROUPS):
            values = vbuf[lax.rem(b, SLOTS), g * run:(g + 1) * run].reshape(run * head, tokens)
            every = lax.dot_general(values, weights[g], (((1,), (1,)), ((), ())), preferred_element_type=jnp.float32)
            own = jnp.zeros((head, run), jnp.float32)
            for h in range(run):
                own = jnp.where(which == h, every[h * head:(h + 1) * head], own)
            sums.append(own.T)
        return sums

    def part(b, sums, stats):
        for g in range(GROUPS):
            send[b, g * run:(g + 1) * run, :] = stats[g]
            send[b, g * run:(g + 1) * run, :head] = sums[g]

    def keep(i, new):
        for g in range(GROUPS):
            weights[i, g], stats[i, g] = new[0][g], new[1][g]

    def kept(i):
        return [weights[i, g] for g in range(GROUPS)], [stats[i, g] for g in range(GROUPS)]

    def scatter(b):
        for h in range(2):
            target = owner_of(b, h)

            @pl.when(target != me)
            def _():
                give(send.at[b, pl.ds(h * half, half)], recv.at[b // 8, lax.rem(me - target + 2 * N - 1, N)],
                     part_send_sem, part_sem.at[b // 8], target).start()

    def combine(r):
        b = 8 * r + my_batch
        pltpu.make_async_copy(recv.at[r], recv.at[r], part_sem.at[r]).wait()
        parts = [send[b, mine, :]] + [recv[r, i] for i in range(N - 1)]
        highs = [p[:, head:head + 1] for p in parts]
        high = functools.reduce(jnp.maximum, highs)
        seen = functools.reduce(jnp.add, [p * jnp.exp(h - high) for p, h in zip(parts, highs)])
        out_ref[b, mine, :] = (seen[:, :head] / seen[:, head + 1:head + 2]).astype(out_ref.dtype)
        for d in range(1, N):
            give(out_ref.at[b, mine], out_ref.at[b, mine], out_send_sem, out_sem, lax.rem(me + d, N)).start()

    q_copy.wait()
    turn(0, 0)
    turn(1, 1)
    for b in range(2):
        fetch(k_hbm, kbuf, ksem, b).wait()
    queries = [turned[0], turned[1]]
    turn(2, 0)
    turn(3, 1)
    for b in range(2):
        keep(b, score(b, queries[b]))
    for b in range(2):
        fetch(k_hbm, kbuf, ksem, SLOTS + b).start(priority=1)

    def work(b, count):
        for j in range(count):
            fetch(k_hbm, kbuf, ksem, b + 2 + j).wait()
            fetch(v_hbm, vbuf, vsem, b + j).wait()
        slots = [lax.rem(b + j, 2) for j in range(count)]
        old = [kept(i) for i in slots]
        queries = [turned[i] for i in slots]
        new, sums = [], []
        for j in range(count):
            new.append(score(b + 2 + j, queries[j]))
            sums.append(see(b + j, old[j][0]))
        for j in range(count):
            turn(b + 4 + j, slots[j])
            part(b + j, sums[j], old[j][1])
            keep(slots[j], new[j])

    def exchange(b, count):
        for j in range(count):
            scatter(b + j)
        for j in range(count):
            @pl.when((b >= 2 * LAG) & (lax.rem(b + j - 2 * LAG + 8, 8) == my_batch))
            def _():
                combine((b + j - 2 * LAG) // 8)

    def step(i, carry):
        b = 2 * i
        work(b, 2)

        @pl.when(b + 2 + SLOTS < batches)
        def _():
            for j in range(2):
                fetch(k_hbm, kbuf, ksem, b + 2 + j + SLOTS).start(priority=1)
                fetch(v_hbm, vbuf, vsem, b + j + SLOTS).start(priority=1)

        @pl.when(b + 2 + SLOTS == batches)
        def _():
            for j in range(2):
                fetch(v_hbm, vbuf, vsem, b + j + SLOTS).start(priority=1)

        @pl.when(i == 0)
        def _():
            pl.semaphore_wait(barrier, N - 1)

        exchange(b, 2)
        return carry

    def single(b, carry):
        work(b, 1)
        exchange(b, 1)
        return carry

    lax.fori_loop(0, (batches - 4) // 2, step, 0)
    lax.fori_loop(batches - 4, batches - TAIL, single, 0)

    @pl.when(my_batch >= 8 - 2 * LAG + 8 - TAIL)
    def _():
        combine(rounds - 2)

    tail = range(batches - TAIL, batches)
    for b in tail:
        fetch(v_hbm, vbuf, vsem, b).wait()
    old = [kept(b % 2) for b in tail]
    sums = [see(b, w) for b, (w, _) in zip(tail, old)]
    for b, y, (_, st) in zip(tail, sums, old):
        part(b, y, st)
    for b in tail:
        scatter(b)

    combine(rounds - 1)

    pltpu.make_async_copy(recv, recv, part_send_sem).wait()
    sent = out_ref.at[pl.ds(0, rounds * (N - 1) // 2)]
    pltpu.make_async_copy(sent, sent, out_sem).wait()
    pltpu.make_async_copy(sent, sent, out_send_sem).wait()


def attend(q, k, v):
    batches, tokens, heads, head = k.shape
    run = heads // GROUPS
    return pl.pallas_call(
        functools.partial(kernel, head ** -0.5),
        out_shape=jax.ShapeDtypeStruct(q.shape, jnp.bfloat16),
        in_specs=[pl.BlockSpec(memory_space=pltpu.HBM)] * 3,
        out_specs=pl.BlockSpec(memory_space=pltpu.VMEM),
        scratch_shapes=[
            pltpu.VMEM(q.shape, jnp.bfloat16),
            pltpu.VMEM((SLOTS, heads, head, tokens), jnp.bfloat16),
            pltpu.VMEM((SLOTS, heads, head, tokens), jnp.bfloat16),
            pltpu.VMEM((run, run * head), jnp.bfloat16),
            pltpu.VMEM((2, heads, LANES), jnp.float32),
            pltpu.VMEM((2, heads, LANES), jnp.bfloat16),
            pltpu.VMEM((2, GROUPS, run, tokens), jnp.bfloat16),
            pltpu.VMEM((2, GROUPS, run, LANES), jnp.float32),
            pltpu.VMEM((batches, heads, LANES), jnp.float32),
            pltpu.VMEM((batches // 8, N - 1, heads // 2, LANES), jnp.float32),
            pltpu.SemaphoreType.DMA,
            pltpu.SemaphoreType.DMA((SLOTS,)),
            pltpu.SemaphoreType.DMA((SLOTS,)),
            pltpu.SemaphoreType.DMA,
            pltpu.SemaphoreType.DMA((batches // 8,)),
            pltpu.SemaphoreType.DMA,
            pltpu.SemaphoreType.DMA,
        ],
        compiler_params=pltpu.CompilerParams(collective_id=0, has_side_effects=True, vmem_limit_bytes=30 * 2**20),
    )(pltpu.with_memory_space_constraint(q, pltpu.HBM), jnp.transpose(k, (0, 2, 3, 1)), jnp.transpose(v, (0, 2, 3, 1)))


def solution(mesh):
    return jax.shard_map(
        attend,
        mesh=mesh,
        in_specs=(P("dp", None, None), P("dp", "sp", None, None), P("dp", "sp", None, None)),
        out_specs=P("dp", None, None),
        check_vma=False,
    )
```
